256 devices in a mesh: band: 32 (over y, z), head: 8 (over x, core).
Axes of the slice: x: 4, y: 4, z: 8, core: 2. Of those that a mesh axis runs over, the one named last changes fastest.
Arguments:
- grid_feat: bfloat16 [524288, 1024], P(('band', 'head')), may hold values from -7 to 7
- mesh_feat: bfloat16 [32768, 1024], P(('band', 'head')), may hold values from -7 to 7
- enc_query: bfloat16 [1024, 1024], replicated, may hold values from -0.1875 to 0.1875
- enc_keyval: bfloat16 [1024, 2048], replicated, may hold values from -0.1875 to 0.1875
- enc_out: bfloat16 [1024, 1024], replicated, may hold values from -0.1875 to 0.1875
- proc_qkv: bfloat16 [3, 1024, 1024], P(None, None, 'head'), may hold values from -0.1875 to 0.1875
- proc_out: bfloat16 [1024, 1024], P('head'), may hold values from -0.1875 to 0.1875
- tile_ids: int32 [512, 8], P(('band', 'head')), may hold values from 0 to 4095, as said below
- key_counts: int32 [512], P(('band', 'head')), may hold values from 128 to 1024, as said below
Outputs:
- mesh_out: bfloat16 [32768, 1024], P(('band', 'head'))
The draws below stay inside these ranges and needn't reach their ends.
Inputs may be any that keep to these rules, and one draw needn't show every extreme that they name: `tile_ids`: mesh tile m lies on the device that holds mesh rows m * 64; every tile it lists is one of that device's grid tiles (grid rows of the same device) or of the 2 grid tiles just before or just after them. Slots may repeat tiles. `key_counts`: the largest value is reached in every draw.
All inputs are finite; a program needn't handle non-finite values.
Results may differ from the reference program's by a relative error of at most 0.012.
The reference program's roundings to bfloat16 on the way count: a program that leaves them out, or rounds other values in their place, can miss the bound.
Values may be sent and summed in bfloat16 or wider, within the bound.
No kernel may reach another device: no remote copies, remote signals or barrier semaphores. Data moves between devices by JAX's collectives and lax.ppermute only.
A program may use at most 128 MiB of HBM per device.

```python
import math
import jax
import jax.numpy as jnp
from jax import lax

D = 1024
HEADS = 16
HALFW = 512
GT = 128
LIST = 8
MT = 64
HALO_TILES = 2
GRID_DEV = 2048
MESH_DEV = 128
GRID = 524288
MESH = 32768


def feature_draw(key, row_count):
    values = jnp.clip(jax.random.normal(key, (row_count, D), jnp.float32), -5.0, 5.0)
    return values.astype(jnp.bfloat16)


def draw_grid_feat(key, part):
    return feature_draw(jax.random.fold_in(key, 11), GRID)


def draw_mesh_feat(key, part):
    return feature_draw(jax.random.fold_in(key, 12), MESH)


def draw_tile_ids(key, part):
    tiles_mesh = MESH // MT
    per_device = MESH_DEV // MT
    tiles_device = GRID_DEV // GT
    owner = jnp.arange(tiles_mesh, dtype=jnp.int32) // per_device
    first_tile = owner * tiles_device - HALO_TILES
    offsets = jax.random.randint(jax.random.fold_in(key, 21), (tiles_mesh, LIST), 0, tiles_device + 2 * HALO_TILES)
    return jnp.clip(first_tile[:, None] + offsets, 0, GRID // GT - 1).astype(jnp.int32)


def draw_key_counts(key, part):
    tiles_mesh = MESH // MT
    counts = jax.random.randint(jax.random.fold_in(key, 31), (tiles_mesh,), GT, LIST * GT + 1)
    position = jax.random.randint(jax.random.fold_in(key, 32), (), 0, tiles_mesh)
    return counts.at[position].set(LIST * GT).astype(jnp.int32)


def block_levels(key, shape, pieces, smallest, largest):
    def one(dim, shards_of):
        heights = jax.random.uniform(jax.random.fold_in(jax.random.fold_in(key, 6), dim), (shards_of,), jnp.float32, smallest / len(pieces), largest / len(pieces))
        return jnp.repeat(jnp.exp(heights), shape[dim] // shards_of).reshape((-1,) + (1,) * (len(shape) - dim - 1))

    level = one(*pieces[0])
    for cut in pieces[1:]:
        level = level * one(*cut)
    return level


def bell_draw(own_key, shape, scale, reach, cuts=(), kind=jnp.bfloat16):
    values = jax.random.normal(own_key, shape, jnp.float32) * scale
    if len(cuts) > 0:
        values = block_levels(own_key, shape, cuts, -0.22, 0.18) * values
    return jnp.clip(values, min=-reach, max=reach).astype(kind)


def setup_inputs(seed: int = 0) -> dict:
    key_of = jax.random.split(jax.random.key(seed), 10)
    grid_feat = draw_grid_feat(jax.random.fold_in(key_of[9], 71), 0)
    mesh_feat = draw_mesh_feat(jax.random.fold_in(key_of[9], 71), 0)
    enc_query = bell_draw(key_of[2], (D, D), D ** -0.5, 0.1875)
    enc_keyval = bell_draw(key_of[3], (D, 2 * D), D ** -0.5, 0.1875)
    enc_out = bell_draw(key_of[4], (D, D), D ** -0.5, 0.1875)
    proc_qkv = bell_draw(key_of[5], (3, D, D), D ** -0.5, 0.1875, ((2, 8),))
    proc_out = bell_draw(key_of[6], (D, D), D ** -0.5, 0.1875, ((0, 8),))
    tile_ids = draw_tile_ids(jax.random.fold_in(key_of[9], 71), 0)
    key_counts = draw_key_counts(jax.random.fold_in(key_of[9], 71), 0)
    return {"grid_feat": grid_feat, "mesh_feat": mesh_feat, "enc_query": enc_query, "enc_keyval": enc_keyval, "enc_out": enc_out, "proc_qkv": proc_qkv, "proc_out": proc_out, "tile_ids": tile_ids, "key_counts": key_counts}


def masked_softmax(scores, key_mask):
    scores = jnp.where(key_mask, scores, -1e30)
    row_top = jnp.max(scores, axis=-1, keepdims=True)
    weights = jnp.exp(scores - row_top)
    return (weights / jnp.sum(weights, axis=-1, keepdims=True)).astype(jnp.bfloat16)


def reference(grid_feat, mesh_feat, enc_query, enc_keyval, enc_out, proc_qkv, proc_out, tile_ids, key_counts):
    head_size = D // HEADS
    score_scale = head_size ** -0.5
    grid_kv = jnp.dot(grid_feat, enc_keyval, preferred_element_type=jnp.float32).astype(jnp.bfloat16)
    grid_tiles = grid_kv.reshape(GRID // GT, GT, 2 * D)
    queries = jnp.dot(mesh_feat, enc_query, preferred_element_type=jnp.float32).astype(jnp.bfloat16)
    positions = jnp.arange(LIST * GT, dtype=jnp.int32)

    def one_tile(packed):
        query_tile, tile_list, valid = packed
        gathered = grid_tiles[tile_list].reshape(LIST * GT, 2 * D)
        key_rows = gathered[:, :D].reshape(LIST * GT, HEADS, head_size).astype(jnp.float32)
        value_rows = gathered[:, D:].reshape(LIST * GT, HEADS, head_size).astype(jnp.float32)
        query_heads = query_tile.reshape(MT, HEADS, head_size).astype(jnp.float32)
        scores = jnp.einsum("qhd,khd->hqk", query_heads, key_rows) * score_scale
        weights = masked_softmax(scores, (positions < valid)[None, None, :])
        attended = jnp.einsum("hqk,khd->qhd", weights.astype(jnp.float32), value_rows)
        return attended.reshape(MT, D).astype(jnp.bfloat16)

    enc_attn = lax.map(one_tile, (queries.reshape(MESH // MT, MT, D), tile_ids, key_counts)).reshape(MESH, D)
    mesh_state = (mesh_feat.astype(jnp.float32) + jnp.dot(enc_attn, enc_out, preferred_element_type=jnp.float32)).astype(jnp.bfloat16)
    query_all = jnp.dot(mesh_state, proc_qkv[0], preferred_element_type=jnp.float32).astype(jnp.bfloat16)
    key_all = jnp.dot(mesh_state, proc_qkv[1], preferred_element_type=jnp.float32).astype(jnp.bfloat16)
    value_all = jnp.dot(mesh_state, proc_qkv[2], preferred_element_type=jnp.float32).astype(jnp.bfloat16)
    padded_keys = jnp.pad(key_all, ((HALFW, HALFW), (0, 0)))
    padded_values = jnp.pad(value_all, ((HALFW, HALFW), (0, 0)))
    block_rows = math.gcd(MESH, 512)

    def one_block(block_index):
        first = block_index * block_rows
        span = block_rows + 2 * HALFW
        query_heads = lax.dynamic_slice_in_dim(query_all, first, block_rows, 0).reshape(block_rows, HEADS, head_size).astype(jnp.float32)
        key_rows = lax.dynamic_slice_in_dim(padded_keys, first, span, 0).reshape(span, HEADS, head_size).astype(jnp.float32)
        value_rows = lax.dynamic_slice_in_dim(padded_values, first, span, 0).reshape(span, HEADS, head_size).astype(jnp.float32)
        query_pos = first + jnp.arange(block_rows, dtype=jnp.int32)
        key_pos = first - HALFW + jnp.arange(span, dtype=jnp.int32)
        near = (jnp.abs(query_pos[:, None] - key_pos[None, :]) < HALFW) & ((key_pos >= 0) & (key_pos < MESH))[None, :]
        scores = jnp.einsum("qhd,khd->hqk", query_heads, key_rows) * score_scale
        weights = masked_softmax(scores, near[None, :, :])
        attended = jnp.einsum("hqk,khd->qhd", weights.astype(jnp.float32), value_rows)
        return attended.reshape(block_rows, D).astype(jnp.bfloat16)

    proc_attn = lax.map(one_block, jnp.arange(MESH // block_rows, dtype=jnp.int32)).reshape(MESH, D)
    return (mesh_state.astype(jnp.float32) + jnp.dot(proc_attn, proc_out, preferred_element_type=jnp.float32)).astype(jnp.bfloat16)
```

```python
import jax
import jax.numpy as jnp
from jax import lax
from jax.experimental import pallas as pl
from jax.experimental.pallas import tpu as pltpu
from jax.sharding import PartitionSpec as P

D = 1024
HEADS = 16
HD = D // HEADS
HALFW = 512
GT = 128
LIST = 8
MT = 64
HALO = 2
BF = jnp.bfloat16
F32 = jnp.float32
NEG = -1e30
SCALE = HD**-0.5
VM = pltpu.VMEM
CP = pltpu.make_async_copy


def dot(a, b):
    return jnp.dot(a, b, preferred_element_type=F32)


def dot_t(a, b):
    return lax.dot_general(a, b, (((1,), (1,)), ((), ())), preferred_element_type=F32)


def spread(q, heads):
    n, w = q.shape
    rows = lax.broadcasted_iota(jnp.int32, (heads * n, w), 0) // n
    cols = lax.broadcasted_iota(jnp.int32, (heads * n, w), 1) // HD
    tall = jnp.concatenate([q.astype(F32) * SCALE] * heads, axis=0)
    return jnp.where(rows == cols, tall, 0.0).astype(BF)


def collect(o, heads):
    n, w = o.shape[0] // heads, o.shape[1]
    cols = lax.broadcasted_iota(jnp.int32, (n, w), 1) // HD
    total = o[:n]
    for h in range(1, heads):
        total = jnp.where(cols == h, o[h * n : (h + 1) * n], total)
    return total


KV_ROWS = 512
KV_COLS = 512


def own_kv_body(x_hbm, w_hbm, out_hbm, xb, wb, ob, sx, sw, so):
    rows, cols = x_hbm.shape[0] // KV_ROWS, w_hbm.shape[1] // KV_COLS

    def x_copy(m):
        at = pl.ds(m * KV_ROWS, KV_ROWS)
        return CP(x_hbm.at[at], xb.at[at], sx.at[m])

    def w_copy(n):
        at = pl.ds(n * KV_COLS, KV_COLS)
        return CP(w_hbm.at[:, at], wb.at[:, at], sw.at[n])

    def o_copy(m):
        at = pl.ds(m * KV_ROWS, KV_ROWS)
        return CP(ob.at[at], out_hbm.at[at], so.at[m])

    x_copy(0).start()
    for n in range(cols):
        w_copy(n).start()
    for m in range(1, rows):
        x_copy(m).start()

    def step(m, carry):
        at = pl.ds(pl.multiple_of(m * KV_ROWS, KV_ROWS), KV_ROWS)
        x_copy(m).wait()
        x = xb[at, :]
        for n in range(cols):

            @pl.when(m == 0)
            def _():
                w_copy(n).wait()

            cut = slice(n * KV_COLS, (n + 1) * KV_COLS)
            ob[at, cut] = dot(x, wb[:, cut]).astype(BF)
        o_copy(m).start()
        return carry

    lax.fori_loop(0, rows, step, 0)
    for m in range(rows):
        o_copy(m).wait()


def own_kv(x, w):
    rows, cols = x.shape[0] // KV_ROWS, w.shape[1] // KV_COLS
    hbm = pl.BlockSpec(memory_space=pltpu.HBM)
    return pl.pallas_call(
        own_kv_body,
        out_shape=jax.ShapeDtypeStruct((x.shape[0], w.shape[1]), BF),
        in_specs=[hbm, hbm],
        out_specs=hbm,
        scratch_shapes=[
            VM(x.shape, BF),
            VM(w.shape, BF),
            VM((x.shape[0], w.shape[1]), BF),
            pltpu.SemaphoreType.DMA((rows,)),
            pltpu.SemaphoreType.DMA((cols,)),
            pltpu.SemaphoreType.DMA((rows,)),
        ],
        cost_estimate=pl.CostEstimate(
            flops=2 * x.shape[0] * w.shape[0] * w.shape[1],
            transcendentals=0,
            bytes_accessed=2 * (x.size + w.size + x.shape[0] * w.shape[1]),
        ),
        name="own_kv",
    )(x, w)


def encode_body(
    ids, counts, kv_hbm, lo_hbm, hi_hbm, w_hbm, mf, wq_hbm, wo_hbm, out, kv, xh, wb, wq, wo, qs, at_s, sem, sw
):
    tiles = kv_hbm.shape[0]
    hr = HALO * GT
    cols = w_hbm.shape[1] // KV_COLS
    c_lo = CP(lo_hbm, xh.at[pl.ds(0, hr)], sem.at[0])
    c_hi = CP(hi_hbm, xh.at[pl.ds(hr, hr)], sem.at[1])
    c_wq = CP(wq_hbm, wq, sem.at[2])
    c_kv = CP(kv_hbm, kv.at[pl.ds(HALO, tiles)], sem.at[3])
    c_wo = CP(wo_hbm, wo, sem.at[4])

    def w_copy(n):
        at = pl.ds(n * KV_COLS, KV_COLS)
        return CP(w_hbm.at[:, at], wb.at[:, at], sw.at[n])

    c_wq.start()
    c_lo.start()
    c_hi.start()
    for n in range(cols):
        w_copy(n).start()
    c_kv.start()
    c_wo.start()
    c_wq.wait()
    qs[...] = dot(mf[...], wq[...]).astype(BF)
    c_lo.wait()
    c_hi.wait()
    for n in range(cols):
        w_copy(n).wait()
        cut = slice(n * KV_COLS, (n + 1) * KV_COLS)
        r = dot(xh[...], wb[:, cut]).astype(BF)
        for t in range(HALO):
            kv[t, :, cut] = r[t * GT : (t + 1) * GT]
            kv[HALO + tiles + t, :, cut] = r[hr + t * GT : hr + (t + 1) * GT]
    first = lax.axis_index(("band", "head")) * tiles - HALO
    c_kv.wait()
    c_wo.wait()
    gw = 4 * HD

    for m in range(mf.shape[0] // MT):
        valid = counts[m]
        at = [ids[m, s] - first for s in range(LIST)]

        for g in range(D // gw):
            q = spread(qs[m * MT : (m + 1) * MT, g * gw : (g + 1) * gw], 4)
            parts = []
            for j in range(LIST // 2):
                k = jnp.concatenate([kv[at[2 * j + i], :, g * gw : (g + 1) * gw] for i in range(2)], axis=0)
                s = dot_t(q, k)
                pos = lax.broadcasted_iota(jnp.int32, s.shape, 1) + 2 * j * GT
                parts.append(jnp.where(pos < valid, s, NEG))
            s = jnp.concatenate(parts, axis=1)
            p = jnp.exp(s - jnp.max(s, axis=1, keepdims=True))
            total = jnp.sum(p, axis=1, keepdims=True)
            p = p.astype(BF)
            o = None
            for j in range(LIST // 2):
                v = jnp.concatenate(
                    [kv[at[2 * j + i], :, D + g * gw : D + (g + 1) * gw] for i in range(2)], axis=0
                )
                part = dot(p[:, 2 * j * GT : 2 * (j + 1) * GT], v)
                o = part if o is None else o + part
            at_s[m * MT : (m + 1) * MT, g * gw : (g + 1) * gw] = collect(o / total, 4).astype(BF)
    out[...] = (mf[...].astype(F32) + dot(at_s[...], wo[...])).astype(BF)


def encode(ids, counts, kv_own, lo, hi, w, mf, wq, wo):
    hbm = pl.BlockSpec(memory_space=pltpu.HBM)
    vm = pl.BlockSpec(memory_space=pltpu.VMEM)
    sm = pl.BlockSpec(memory_space=pltpu.SMEM)
    tiles = kv_own.shape[0]
    return pl.pallas_call(
        encode_body,
        out_shape=jax.ShapeDtypeStruct(mf.shape, BF),
        in_specs=[sm, sm, hbm, hbm, hbm, hbm, vm, hbm, hbm],
        out_specs=vm,
        scratch_shapes=[
            VM((tiles + 2 * HALO, GT, 2 * D), BF),
            VM((2 * HALO * GT, D), BF),
            VM(w.shape, BF),
            VM(wq.shape, BF),
            VM(wo.shape, BF),
            VM(mf.shape, BF),
            VM(mf.shape, BF),
            pltpu.SemaphoreType.DMA((5,)),
            pltpu.SemaphoreType.DMA((w.shape[1] // KV_COLS,)),
        ],
        cost_estimate=pl.CostEstimate(flops=12 * 10**9, transcendentals=2 * 10**6, bytes_accessed=16 * 2**20),
        name="encode",
    )(ids, counts, kv_own, lo, hi, w, mf, wq, wo)


def sources(h):
    n = lax.axis_size("head")
    p = h ^ 1
    return [h, (h + n - 2) % n, (h + 2) % n, (h + 4) % n, p, (p + n - 2) % n, (p + 2) % n, (p + 4) % n]


def ring_exchange(x):
    n = lax.axis_size("head")
    right = [(i, (i + 2) % n) for i in range(n)]
    left = [(i, (i - 2) % n) for i in range(n)]
    flip = [(i, i ^ 1) for i in range(n)]
    half = x.shape[0] // 2
    r1 = lax.ppermute(x, "head", right)
    l1 = lax.ppermute(x, "head", left)
    o0 = lax.ppermute(x, "head", flip)
    a = lax.ppermute(r1[:half], "head", right)
    b = lax.ppermute(l1[half:], "head", left)
    o1 = lax.ppermute(jnp.concatenate([r1, l1], axis=0), "head", flip)
    o2 = lax.ppermute(jnp.concatenate([a, b], axis=0), "head", flip)
    return [x, r1, l1, a, b, o0, o1, o2]


def gather_rows(refs):
    x, r1, l1, a, b, o0, o1, o2 = refs
    return jnp.concatenate([r[...] for r in (x, r1, l1, a, b, o0, o1, o2)], axis=0)


def qkv_body(x, r1, l1, a, b, o0, o1, o2, w, q_out, kva, kvb, kv):
    rows = gather_rows((x, r1, l1, a, b, o0, o1, o2))
    n = x.shape[0]
    wqk = jnp.concatenate([w[0], w[1]], axis=1)
    qk = dot(rows, wqk).astype(BF)
    v = dot(rows, w[2]).astype(BF)
    hc = w.shape[2]
    for i, place in enumerate(sources(lax.axis_index("head"))):
        at = pl.ds(pl.multiple_of(place * n, n), n)
        q_out[at, :] = qk[i * n : (i + 1) * n, :hc]
        kv[at, :hc] = qk[i * n : (i + 1) * n, hc:]
        kv[at, hc:] = v[i * n : (i + 1) * n]
    half = kva.shape[0]
    kva[...] = kv[:half]
    kvb[...] = kv[half:]


def project_qkv(pieces, w):
    n, hc = pieces[0].shape[0], w.shape[2]
    group = n * lax.axis_size("head")
    half = jax.ShapeDtypeStruct((group // 2, 2 * hc), BF)
    return pl.pallas_call(
        qkv_body,
        out_shape=(jax.ShapeDtypeStruct((group, hc), BF), half, half),
        scratch_shapes=[VM((group, 2 * hc), BF)],
        cost_estimate=pl.CostEstimate(flops=6 * group * D * hc, transcendentals=0, bytes_accessed=4 * 2**20),
        name="qkv",
    )(*pieces, w)


QB = 128


def window_body(q, lo, kva, kvb, hi, out, kv):
    hc = q.shape[1]
    heads = hc // HD
    for i, r in enumerate((lo, kva, kvb, hi)):
        kv[i * HALFW : (i + 1) * HALFW] = r[...]
    band = lax.axis_index("band")
    bands = lax.axis_size("band")
    has_lo = band > 0
    has_hi = band < bands - 1
    side = HALFW // QB
    blocks = q.shape[0] // QB
    row = lax.broadcasted_iota(jnp.int32, (heads * QB, QB), 0) % QB
    col = lax.broadcasted_iota(jnp.int32, (heads * QB, QB), 1)
    for n in range(blocks):
        qn = spread(q[n * QB : (n + 1) * QB], heads)
        span = slice(n * QB, (n + 2 * side + 1) * QB)
        s = dot_t(qn, kv[span, :hc])
        parts = []
        for c in range(2 * side + 1):
            part = s[:, c * QB : (c + 1) * QB]
            ok = None
            if c == 0:
                ok = col > row
            if c == 2 * side:
                ok = col < row
            if n + c < side:
                ok = has_lo if ok is None else jnp.logical_and(ok, has_lo)
            if n + c >= side + blocks:
                ok = has_hi if ok is None else jnp.logical_and(ok, has_hi)
            parts.append(part if ok is None else jnp.where(ok, part, NEG))
        s = jnp.concatenate(parts, axis=1)
        p = jnp.exp(s - jnp.max(s, axis=1, keepdims=True))
        total = jnp.sum(p, axis=1, keepdims=True)
        o = dot(p.astype(BF), kv[span, hc:])
        out[n] = collect(o / total, heads).astype(BF)


def window(q, lo, kva, kvb, hi):
    group, hc = q.shape
    return pl.pallas_call(
        window_body,
        out_shape=jax.ShapeDtypeStruct((group // QB, QB, hc), BF),
        scratch_shapes=[VM((group + 2 * HALFW, 2 * hc), BF)],
        cost_estimate=pl.CostEstimate(flops=2 * 10**9, transcendentals=2 * 10**6, bytes_accessed=2 * 2**20),
        name="window",
    )(q, lo, kva, kvb, hi)


def finish_body(at, ms, x, r1, l1, a, b, o0, o1, o2, out):
    rows = gather_rows((x, r1, l1, a, b, o0, o1, o2))
    att = jnp.concatenate([at[place] for place in sources(lax.axis_index("head"))], axis=1)
    out[...] = (ms[...].astype(F32) + dot(att, rows)).astype(BF)


def finish(attn, state, pieces):
    return pl.pallas_call(
        finish_body,
        out_shape=jax.ShapeDtypeStruct(state.shape, BF),
        cost_estimate=pl.CostEstimate(flops=2 * state.size * D, transcendentals=0, bytes_accessed=3 * 2**20),
        name="finish",
    )(attn, state, *pieces)


def local(grid_feat, mesh_feat, enc_query, enc_keyval, enc_out, proc_qkv, proc_out, tile_ids, key_counts):
    tiles = grid_feat.shape[0] // GT
    both = ("band", "head")
    size = lax.axis_size(both)
    up = [(i, i + 1) for i in range(size - 1)]
    down = [(b, a) for a, b in up]
    lo = lax.ppermute(grid_feat[-HALO * GT :], both, up)
    hi = lax.ppermute(grid_feat[: HALO * GT], both, down)
    out_pieces = ring_exchange(proc_out)
    kv_own = own_kv(grid_feat, enc_keyval).reshape(tiles, GT, 2 * D)
    state = encode(tile_ids, key_counts, kv_own, lo, hi, enc_keyval, mesh_feat, enc_query, enc_out)
    q, kva, kvb = project_qkv(ring_exchange(state), proc_qkv)
    bands = lax.axis_size("band")
    b_up = [(i, i + 1) for i in range(bands - 1)]
    b_down = [(b, a) for a, b in b_up]
    k_lo = lax.ppermute(kvb, "band", b_up)
    k_hi = lax.ppermute(kva, "band", b_down)
    attn = window(q, k_lo, kva, kvb, k_hi)
    attn = lax.all_to_all(attn, "head", split_axis=0, concat_axis=0, tiled=True)
    return finish(attn, state, out_pieces)


def solution(mesh):
    rows = P(("band", "head"), None)
    return jax.shard_map(
        local,
        mesh=mesh,
        in_specs=(
            rows,
            rows,
            P(),
            P(),
            P(),
            P(None, None, "head"),
            P("head", None),
            rows,
            P(("band", "head")),
        ),
        out_specs=rows,
        check_vma=False,
    )
```
